32 devices in a mesh: dp: 4 (over y, x), seq: 8 (over z, core).
Axes of the slice: x: 2, y: 2, z: 4, core: 2. Of those that a mesh axis runs over, the one named last changes fastest.
Arguments:
- layer_input: bfloat16 [2, 4, 1024, 1600], P(None, 'dp', 'seq'), may hold values from -3 to 3
- cotangent: bfloat16 [2, 4, 1024, 1600], P(None, 'dp', 'seq'), may hold values from -1.5 to 1.5
- block_order: int32 [16], replicated, may hold values from 0 to 15, as said below
- w_qkv: bfloat16 [1600, 4800], P('dp', 'seq'), may hold values from -0.15625 to 0.15625
- w_out: bfloat16 [1600, 1600], P('dp', 'seq'), may hold values from -1.75 to 1.75
- w_up: bfloat16 [1600, 6400], P('dp', 'seq'), may hold values from -0.15625 to 0.15625
- w_down: bfloat16 [6400, 1600], P('dp', 'seq'), may hold values from -0.078125 to 0.078125
- vectors: bfloat16 [12, 1600], P('dp', 'seq'), may hold values from -2 to 2
Outputs:
- output: bfloat16 [2, 4, 1024, 1600], P(None, 'dp', 'seq')
- grad_input: bfloat16 [2, 4, 1024, 1600], P(None, 'dp', 'seq')
- grad_w_qkv: float32 [1600, 4800], P('dp', 'seq')
- grad_w_out: float32 [1600, 1600], P('dp', 'seq')
- grad_w_up: float32 [1600, 6400], P('dp', 'seq')
- grad_w_down: float32 [6400, 1600], P('dp', 'seq')
- grad_vectors: float32 [12, 1600], P('dp', 'seq')
The draws below stay inside these ranges and needn't reach their ends.
Inputs may be any that keep to these rules, and one draw needn't show every extreme that they name: block_order holds every block number once; its entries 2i and 2i + 1 sum to 15, and entry 2i is below 8.
All inputs are finite; a program needn't handle non-finite values.
Results may differ from the reference program's by a relative error of at most 0.018.
Values may be sent and summed in bfloat16 or wider, within the bound.
A program may use at most 448 MiB of HBM per device.

```python
import jax
import jax.numpy as jnp
from jax import lax

D = 1600
FF = 6400
HEADS = 25
HEAD_DIM = 64
MICRO = 2
BLOCK_TOK = 64
BLOCKS = 16
LEN = 1024
N_DP = 4
N_SEQ = 8


def draw_layer_input(key, part):
    base_key, row_key, column_key = jax.random.split(key, 3)
    shape = (MICRO, N_DP, LEN, D)
    row_scale = jnp.exp(jax.random.uniform(row_key, (MICRO, N_DP, LEN, 1), jnp.float32, -0.4, 0.4))
    column_scale = jnp.exp(jax.random.uniform(column_key, (D,), jnp.float32, -0.4, 0.4))
    base = 0.4 * jnp.clip(jax.random.normal(base_key, shape, jnp.float32), -3.0, 3.0)
    values = base * row_scale * column_scale
    return values.astype(jnp.bfloat16)


def draw_vectors(key, part):
    gain_key, other_key = jax.random.split(key, 2)
    row_ids = jnp.arange(12)[:, None]
    is_gain = (row_ids == 0) | (row_ids == 2)
    spread = jnp.where(row_ids == 5, 0.05, jnp.where(row_ids >= 8, 0.5, 0.3))
    gains = 1.0 + jnp.clip(0.15 * jax.random.normal(gain_key, (12, D), jnp.float32), -0.6, 0.6)
    others = jnp.clip(jax.random.normal(other_key, (12, D), jnp.float32), -3.5, 3.5) * spread
    return jnp.where(is_gain, gains, others).astype(jnp.bfloat16)


def draw_block_order(key, part):
    order = jax.random.permutation(key, N_SEQ).astype(jnp.int32)
    paired = jnp.stack([order, BLOCKS - 1 - order], axis=1)
    return paired.reshape(BLOCKS).astype(jnp.int32)


def steps_of(own_key, dims, pieces, smallest, largest):
    level = 1.0
    for dim, blocks in pieces:
        steps = jax.random.uniform(jax.random.fold_in(jax.random.fold_in(own_key, 6), dim), (blocks,), jnp.float32, smallest / len(pieces), largest / len(pieces))
        level = level * jnp.repeat(jnp.exp(steps), dims[dim] // blocks).reshape((-1,) + (1,) * (len(dims) - 1 - dim))
    return level


def gaussian(stream_key, dims, scale, limit, cuts=(), kind=jnp.bfloat16):
    entries = scale * jax.random.normal(stream_key, dims, jnp.float32)
    if cuts:
        entries = entries * steps_of(stream_key, dims, cuts, -0.22, 0.18)
    return jnp.clip(entries, -limit, limit).astype(kind)


def setup_inputs(seed: int = 0) -> dict:
    seeds = jax.random.split(jax.random.key(seed), 9)
    return {
        "layer_input": draw_layer_input(jax.random.fold_in(seeds[8], 71), 0),
        "cotangent": gaussian(seeds[1], (MICRO, N_DP, LEN, D), 0.25, 1.5, ((1, 4), (2, 8))),
        "block_order": draw_block_order(jax.random.fold_in(seeds[8], 71), 0),
        "w_qkv": gaussian(seeds[3], (D, 3 * D), D ** -0.5, 0.15625, ((0, 4), (1, 8))),
        "w_out": gaussian(seeds[4], (D, D), (max(1, 8 * D // LEN)) ** -0.5, 1.75, ((0, 4), (1, 8))),
        "w_up": gaussian(seeds[5], (D, FF), D ** -0.5, 0.15625, ((0, 4), (1, 8))),
        "w_down": gaussian(seeds[6], (FF, D), FF ** -0.5, 0.078125, ((0, 4), (1, 8))),
        "vectors": draw_vectors(jax.random.fold_in(seeds[8], 71), 0),
    }


EPSILON = 1e-05
SCALE = 0.125
CUBIC = 0.044715
ROOT_TWO_PI = 0.7978845608028654
HIGH = lax.Precision.HIGHEST

@jax.custom_vjp
def low(v):
    return lax.optimization_barrier(v.astype(jnp.bfloat16)).astype(jnp.float32)

@jax.custom_vjp
def low_back(v):
    return v

def low_keep(v):
    return (low(v), None)

def low_pass(kept, grad):
    return (grad,)

def back_keep(v):
    return (v, None)

def back_low(kept, grad):
    return (low(grad),)
low.defvjp(low_keep, low_pass)
low_back.defvjp(back_keep, back_low)

def gelu_tanh(values):
    return 0.5 * values * (1.0 + jnp.tanh(ROOT_TWO_PI * (values + CUBIC * values * values * values)))

def norm(values, gain, shift):
    center = values - lax.optimization_barrier(jnp.mean(values, axis=-1, keepdims=True))
    return center * lax.rsqrt(lax.optimization_barrier(jnp.mean(center * center, axis=-1, keepdims=True)) + EPSILON) * gain + shift

def attend_rows(pair, keys, values, key_positions):
    queries, query_positions = pair
    scores = jnp.einsum('qhd,khd->hqk', queries, keys, precision=HIGH) * SCALE
    scores = low_back(scores)
    visible = key_positions[None, None, :] <= query_positions[None, :, None]
    scores = jnp.where(visible, scores, -1e+30)
    peak = lax.optimization_barrier(jnp.max(scores, axis=-1, keepdims=True))
    raised = jnp.exp(scores - peak)
    weights = low(raised / lax.optimization_barrier(jnp.sum(raised, axis=-1, keepdims=True)))
    return jnp.einsum('hqk,khd->qhd', weights, values, precision=HIGH)

def forward(tokens, w_qkv, w_out, w_up, w_down, vectors, positions):
    entry_one = low(norm(tokens, vectors[0], vectors[1]))
    joined = jnp.dot(entry_one, w_qkv, precision=HIGH, preferred_element_type=jnp.float32)
    queries = low(low_back(joined[:, :D] + vectors[4]))
    keys = low(low_back(joined[:, D:2 * D]))
    values = low(low_back(joined[:, 2 * D:] + vectors[5]))
    rows_block = min(512, LEN)
    query_blocks = queries.reshape(LEN // rows_block, rows_block, HEADS, HEAD_DIM)
    position_blocks = positions.reshape(LEN // rows_block, rows_block)
    head_keys = keys.reshape(LEN, HEADS, HEAD_DIM)
    head_values = values.reshape(LEN, HEADS, HEAD_DIM)
    step = jax.checkpoint(lambda pair: attend_rows(pair, head_keys, head_values, positions))
    mixed = lax.map(step, (query_blocks, position_blocks)).reshape(LEN, D)
    mixed = low(low_back(mixed))
    middle = tokens + low_back(jnp.dot(mixed, w_out, precision=HIGH, preferred_element_type=jnp.float32) + vectors[6])
    entry_two = low(norm(middle, vectors[2], vectors[3]))
    hidden_pre = low_back(jnp.dot(entry_two, w_up, precision=HIGH, preferred_element_type=jnp.float32) + vectors[8:].reshape(FF))
    hidden = low(gelu_tanh(hidden_pre))
    return middle + low_back(jnp.dot(hidden, w_down, precision=HIGH, preferred_element_type=jnp.float32) + vectors[7])

def reference(layer_input, cotangent, block_order, w_qkv, w_out, w_up, w_down, vectors):
    params = (w_qkv.astype(jnp.float32), w_out.astype(jnp.float32), w_up.astype(jnp.float32), w_down.astype(jnp.float32), vectors.astype(jnp.float32))
    token_ids = jnp.arange(LEN, dtype=jnp.int32)
    positions = block_order[token_ids // BLOCK_TOK].astype(jnp.int32) * BLOCK_TOK + token_ids % BLOCK_TOK
    seq_inputs = layer_input.reshape(MICRO * N_DP, LEN, D)
    seq_cotangents = cotangent.reshape(MICRO * N_DP, LEN, D)

    def apply(tokens, matrix_qkv, matrix_out, matrix_up, matrix_down, table):
        return forward(tokens, matrix_qkv, matrix_out, matrix_up, matrix_down, table, positions)

    def one_sequence(totals, item):
        seq_in, seq_cot = item
        result, pull = jax.vjp(apply, seq_in.astype(jnp.float32), params[0], params[1], params[2], params[3], params[4])
        grads = pull(seq_cot.astype(jnp.float32))
        totals = tuple((left + right for left, right in zip(totals, grads[1:])))
        return (totals, (result.astype(jnp.bfloat16), grads[0].astype(jnp.bfloat16)))
    start = tuple((jnp.zeros(matrix.shape, jnp.float32) for matrix in params))
    totals, (outputs, grad_inputs) = lax.scan(one_sequence, start, (seq_inputs, seq_cotangents))
    return (outputs.reshape(layer_input.shape), grad_inputs.reshape(layer_input.shape), totals[0], totals[1], totals[2], totals[3], totals[4])
```

```python
import functools

import jax
import jax.numpy as jnp
from jax import lax
from jax.experimental import pallas as pl
from jax.experimental.pallas import tpu as pltpu
from jax.sharding import PartitionSpec as P

HEAD_DIM = 64
EPSILON = 1e-05
SCALE = 0.125
CUBIC = 0.044715
ROOT_TWO_PI = 0.7978845608028654
F32 = jnp.float32
BF16 = jnp.bfloat16


def dot(left, right, dims):
    return lax.dot_general(left, right, (dims, ((), ())), preferred_element_type=F32)


NN = ((1,), (0,))
NT = ((1,), (1,))
TN = ((0,), (0,))


def gelu_tanh(values):
    return (
        0.5 * values * (1.0 + jnp.tanh(ROOT_TWO_PI * (values + CUBIC * values * values * values)))
    )


def norm_forward(values, gain, shift):
    center = values - jnp.mean(values, axis=-1, keepdims=True)
    scale = lax.rsqrt(jnp.mean(center * center, axis=-1, keepdims=True) + EPSILON)
    normed = center * scale
    return (normed * gain + shift, normed, scale)


def norm_backward(grad_out, normed, scale, gain):
    scaled = grad_out * gain
    first = jnp.mean(scaled, axis=-1, keepdims=True)
    second = jnp.mean(scaled * normed, axis=-1, keepdims=True)
    return (
        scale * (scaled - first - normed * second),
        jnp.sum(grad_out * normed, axis=0),
        jnp.sum(grad_out, axis=0),
    )


def to_natural(order_ref, source, target, block):
    for slot in range(source.shape[0] // block):
        start = pl.multiple_of(order_ref[slot] * block, block)
        target[pl.ds(start, block), :] = source[slot * block : (slot + 1) * block, :]


def to_layout(order_ref, source, target, block):
    for slot in range(source.shape[0] // block):
        start = pl.multiple_of(order_ref[slot] * block, block)
        target[slot * block : (slot + 1) * block, :] = source[pl.ds(start, block), :].astype(
            target.dtype
        )


def causal(scores, tile):
    keys = lax.broadcasted_iota(jnp.int32, (tile, tile), 0)
    queries = lax.broadcasted_iota(jnp.int32, (tile, tile), 1)
    edge = jnp.where(keys <= queries, scores[-tile:, :], -1e30)
    if scores.shape[0] == tile:
        return edge
    return jnp.concatenate([scores[:-tile, :], edge], axis=0)


def attend_kernel(heads, block, tile, order_ref, joined_ref, mixed_ref, level_ref, natural, out):
    length = joined_ref.shape[0]
    span = heads * HEAD_DIM
    to_natural(order_ref, joined_ref, natural, block)
    for head in range(heads):
        low, high = head * HEAD_DIM, (head + 1) * HEAD_DIM
        values_t = natural[:, 2 * span + low : 2 * span + high].T
        for start in range(0, length, tile):
            total = start + tile
            queries = natural[start:total, low:high]
            keys = natural[:total, span + low : span + high]
            scores = causal(dot(keys, queries, NT) * SCALE, tile)
            peak = jnp.max(scores, axis=0, keepdims=True)
            raised = jnp.exp(scores - peak)
            summed = jnp.sum(raised, axis=0, keepdims=True)
            weights = (raised * (1.0 / summed)).astype(BF16)
            part = dot(values_t[:, :total], weights, NN)
            out[start:total, low:high] = part.T
            level_ref[head : head + 1, start:total] = peak + jnp.log(summed)
    to_layout(order_ref, out, mixed_ref, block)


def attend_back_kernel(
    heads, block, tile, order_ref, joined_ref, grad_ref, level_ref, result_ref,
    natural, grads, out, keys_sum, values_sum,
):
    length = joined_ref.shape[0]
    span = heads * HEAD_DIM
    to_natural(order_ref, joined_ref, natural, block)
    to_natural(order_ref, grad_ref, grads, block)
    for head in range(heads):
        low, high = head * HEAD_DIM, (head + 1) * HEAD_DIM
        keys_all = natural[:, span + low : span + high]
        values_all = natural[:, 2 * span + low : 2 * span + high]
        keys_t = keys_all.T
        for start in reversed(range(0, length, tile)):
            total = start + tile
            queries = natural[start:total, low:high]
            grad_part = grads[start:total, low:high]
            scores = causal(dot(keys_all[:total], queries, NT) * SCALE, tile)
            weights = jnp.exp(scores - level_ref[head : head + 1, start:total])
            grad_weights = dot(values_all[:total], grad_part, NT)
            offset = jnp.sum(weights * grad_weights, axis=0, keepdims=True)
            grad_scores = (weights * (grad_weights - offset)).astype(BF16)
            values_term = dot(weights.astype(BF16), grad_part, NN)
            keys_term = dot(grad_scores, queries, NN)
            query_term = dot(keys_t[:, :total], grad_scores, NN)
            out[start:total, low:high] = query_term.T * SCALE
            if total == length:
                keys_sum[...] = keys_term
                values_sum[...] = values_term
            else:
                keys_sum[:total, :] += keys_term
                values_sum[:total, :] += values_term
        out[:, span + low : span + high] = keys_sum[...] * SCALE
        out[:, 2 * span + low : 2 * span + high] = values_sum[...]
    to_layout(order_ref, out, result_ref, block)


VMEM_SPEC = pl.BlockSpec(memory_space=pltpu.VMEM)
SMEM_SPEC = pl.BlockSpec(memory_space=pltpu.SMEM)


def attend(order, joined, heads, block):
    length, span = joined.shape[0], heads * HEAD_DIM
    tile = min(256, length)
    pairs = heads * length * (length + tile) // 2
    return pl.pallas_call(
        functools.partial(attend_kernel, heads, block, tile),
        out_shape=(
            jax.ShapeDtypeStruct((length, span), BF16),
            jax.ShapeDtypeStruct((heads, length), F32),
        ),
        in_specs=[SMEM_SPEC, VMEM_SPEC],
        out_specs=(VMEM_SPEC, VMEM_SPEC),
        scratch_shapes=[pltpu.VMEM((length, 3 * span), BF16), pltpu.VMEM((length, span), F32)],
        cost_estimate=pl.CostEstimate(
            flops=pairs * 256, transcendentals=pairs, bytes_accessed=length * span * 8
        ),
        name="attend",
    )(order, joined)


def attend_back(order, joined, grad_mixed, level, heads, block):
    length, span = joined.shape[0], heads * HEAD_DIM
    tile = min(256, length)
    pairs = heads * length * (length + tile) // 2
    return pl.pallas_call(
        functools.partial(attend_back_kernel, heads, block, tile),
        out_shape=jax.ShapeDtypeStruct((length, 3 * span), BF16),
        in_specs=[SMEM_SPEC, VMEM_SPEC, VMEM_SPEC, VMEM_SPEC],
        out_specs=VMEM_SPEC,
        scratch_shapes=[
            pltpu.VMEM((length, 3 * span), BF16),
            pltpu.VMEM((length, span), BF16),
            pltpu.VMEM((length, 3 * span), F32),
            pltpu.VMEM((length, HEAD_DIM), F32),
            pltpu.VMEM((length, HEAD_DIM), F32),
        ],
        cost_estimate=pl.CostEstimate(
            flops=pairs * 640, transcendentals=pairs, bytes_accessed=length * span * 14
        ),
        name="attend_back",
    )(order, joined, grad_mixed, level)


def shards(layer_input, cotangent, block_order, w_qkv, w_out, w_up, w_down, vectors):
    n_dp, n_seq = lax.axis_size("dp"), lax.axis_size("seq")
    dp, seq = lax.axis_index("dp"), lax.axis_index("seq")
    micro, local, per, width = layer_input.shape
    block = per // 2
    length = per * n_seq
    tokens = micro * local * per
    sequences = n_dp * micro * local
    ff_local = w_up.shape[1]
    ff_piece = ff_local // n_dp
    d_row, d_col = w_qkv.shape[0], w_out.shape[1]
    heads_all = width // HEAD_DIM
    groups = n_seq // sequences
    heads = -(-heads_all // (n_dp * groups))
    padded = n_dp * groups * heads
    span = heads * HEAD_DIM
    wide = groups * 3 * span

    def gather(x, axis, dim=0):
        return lax.all_gather(x, axis, axis=dim, tiled=True)

    def scatter(x, axis, dim=0):
        return lax.psum_scatter(x.astype(BF16), axis, scatter_dimension=dim, tiled=True)

    def swap(x, axis):
        return lax.all_to_all(x, axis, 0, 0, tiled=True)

    small = gather(gather(vectors, "dp"), "seq", 1)
    table = small.astype(F32)

    qkv_rows = gather(w_qkv[None], "seq")
    qkv_rows = qkv_rows.transpose(1, 0, 2).reshape(d_row, 3, heads_all, HEAD_DIM)
    qkv_rows = jnp.pad(qkv_rows, ((0, 0), (0, 0), (0, padded - heads_all), (0, 0)))
    qkv_rows = qkv_rows.reshape(d_row, 3, n_dp, groups, span).transpose(2, 0, 3, 1, 4)
    qkv = swap(qkv_rows.reshape(n_dp, d_row, wide), "dp").reshape(width, wide)

    up_send = w_up.T.reshape(n_dp, ff_piece, d_row)
    down_send = w_down.T.reshape(d_col, n_seq // n_dp, n_dp, ff_piece).transpose(2, 0, 1, 3)
    down_send = down_send.reshape(n_dp, d_col, -1)
    up_part = swap(up_send, "dp").transpose(1, 0, 2).reshape(ff_piece, width)
    down_part = swap(down_send, "dp").transpose(1, 0, 2).reshape(d_col, -1)
    up_t = gather(up_part, "seq")
    down_t = gather(down_part, "seq")

    out_t = gather(gather(w_out.T, "seq")[None], "dp").transpose(1, 0, 2).reshape(width, width)

    def bias_heads(rows):
        rows = jnp.pad(rows.reshape(heads_all, HEAD_DIM), ((0, padded - heads_all), (0, 0)))
        rows = rows.reshape(n_dp, groups, span)
        return lax.dynamic_index_in_dim(rows, dp, 0, keepdims=False)

    nothing = jnp.zeros((groups, span), F32)
    qkv_bias = jnp.stack([bias_heads(table[4]), nothing, bias_heads(table[5])], axis=1)
    qkv_bias = qkv_bias.reshape(1, wide)
    up_bias = table[8:].reshape(n_seq, n_dp, ff_piece)
    up_bias = lax.dynamic_index_in_dim(up_bias, dp, 1, keepdims=False).reshape(1, -1)

    def to_sequences(x):
        columns = x.shape[-1] // groups
        x = x.reshape(sequences, per, groups, columns).transpose(0, 2, 1, 3)
        return swap(x.reshape(n_seq, per, columns), "seq").reshape(length, columns)

    def to_tokens(x):
        columns = x.shape[-1]
        x = swap(x.reshape(n_seq, per, columns), "seq")
        x = x.reshape(sequences, groups, per, columns).transpose(0, 2, 1, 3)
        return x.reshape(n_dp * tokens, groups * columns)

    residual = layer_input.reshape(tokens, width).astype(F32)
    cot = cotangent.reshape(tokens, width)
    entry_one, first_norm, first_scale = norm_forward(residual, table[0], table[1])
    entries_one = gather(entry_one.astype(BF16), "dp")
    cots = gather(cot, "dp")
    joined = (dot(entries_one, qkv, NN) + qkv_bias).astype(BF16)
    joined = to_sequences(joined)
    mixed, level = attend(block_order, joined, heads, block)

    mixed = swap(to_tokens(mixed).reshape(n_dp, tokens, groups * span), "dp")
    mixed = mixed.transpose(1, 0, 2).reshape(tokens, padded * HEAD_DIM)[:, :width]
    middle = residual + dot(mixed, out_t, NT) + table[6]
    entry_two, second_norm, second_scale = norm_forward(middle, table[2], table[3])
    entries_two = gather(entry_two.astype(BF16), "dp")
    hidden_pre = dot(entries_two, up_t, NT) + up_bias
    hidden = gelu_tanh(hidden_pre).astype(BF16)
    branch = scatter(dot(hidden, down_t, NT), "dp").astype(F32)
    output = (middle + branch + table[7]).astype(BF16)

    cot_wide = cot.astype(F32)
    grad_hidden = dot(cots, down_t, NN)
    ignored, pull = jax.vjp(gelu_tanh, hidden_pre)
    grad_pre = pull(grad_hidden)[0].astype(BF16)
    grad_entry_two = scatter(dot(grad_pre, up_t, NN), "dp").astype(F32)
    grad_down_t = scatter(dot(cots, hidden, TN), "seq")
    grad_up_t = scatter(dot(grad_pre, entries_two, TN), "seq")
    grad_middle, grad_gain_two, grad_shift_two = norm_backward(
        grad_entry_two, second_norm, second_scale, table[2]
    )
    grad_middle = grad_middle + cot_wide
    grad_branch = grad_middle.astype(BF16)
    grad_mixed = dot(grad_branch, out_t, NN).astype(BF16)
    grad_mixed = jnp.pad(grad_mixed, ((0, 0), (0, padded * HEAD_DIM - width)))
    grad_mixed = grad_mixed.reshape(tokens, n_dp, groups * span).transpose(1, 0, 2)
    grad_mixed = to_sequences(swap(grad_mixed, "dp"))
    grad_out = scatter(scatter(dot(mixed, grad_branch, TN), "dp").T, "seq")

    grad_joined = attend_back(block_order, joined, grad_mixed, level, heads, block)
    grad_joined = to_tokens(grad_joined)
    grad_entry_one = scatter(dot(grad_joined, qkv, NT), "dp").astype(F32)
    grad_qkv = dot(entries_one, grad_joined, TN).astype(BF16)
    grad_qkv = swap(grad_qkv.reshape(n_dp, d_row, wide), "dp")
    grad_qkv = grad_qkv.reshape(n_dp, d_row, groups, 3, span).transpose(1, 3, 0, 2, 4)
    grad_qkv = grad_qkv.reshape(d_row, 3, padded * HEAD_DIM)[:, :, :width]
    grad_qkv = grad_qkv.reshape(d_row, n_seq, -1).transpose(1, 0, 2)
    grad_qkv = scatter(grad_qkv, "seq").reshape(d_row, -1)

    grad_residual, grad_gain_one, grad_shift_one = norm_backward(
        grad_entry_one, first_norm, first_scale, table[0]
    )
    grad_input = (grad_residual + grad_middle).astype(BF16)

    grad_up = swap(grad_up_t.reshape(ff_piece, n_dp, d_row).transpose(1, 0, 2), "dp")
    grad_up = grad_up.reshape(ff_local, d_row).T
    grad_down = swap(grad_down_t.reshape(d_col, n_dp, -1).transpose(1, 0, 2), "dp")
    grad_down = grad_down.reshape(n_dp, d_col, n_seq // n_dp, ff_piece).transpose(2, 0, 3, 1)
    grad_down = grad_down.reshape(w_down.shape)

    own = (jnp.arange(n_dp) == dp).astype(F32)
    joined_sum = jnp.sum(grad_joined.astype(F32), axis=0).reshape(1, groups, 3, span)
    joined_sum = (own[:, None, None, None] * joined_sum).transpose(2, 0, 1, 3)
    joined_sum = joined_sum.reshape(3, padded * HEAD_DIM)[:, :width]
    up_sum = jnp.sum(grad_pre.astype(F32), axis=0).reshape(n_seq, 1, ff_piece)
    up_sum = (own[None, :, None] * up_sum).reshape(-1, width)
    rows = jnp.stack(
        [
            grad_gain_one,
            grad_shift_one,
            grad_gain_two,
            grad_shift_two,
            joined_sum[0],
            joined_sum[2],
            jnp.sum(grad_branch.astype(F32), axis=0),
            jnp.sum(cot_wide, axis=0),
        ]
    )
    rows = lax.psum(jnp.concatenate([rows, up_sum], axis=0), ("dp", "seq"))
    grad_vectors = lax.dynamic_slice(
        rows, (dp * vectors.shape[0], seq * vectors.shape[1]), vectors.shape
    )
    return (
        output.reshape(layer_input.shape),
        grad_input.reshape(layer_input.shape),
        grad_qkv.astype(F32),
        grad_out.T.astype(F32),
        grad_up.astype(F32),
        grad_down.astype(F32),
        grad_vectors,
    )


def solution(mesh):
    both = P(None, "dp", "seq", None)
    matrix = P("dp", "seq")
    return jax.shard_map(
        shards,
        mesh=mesh,
        in_specs=(both, both, P(), matrix, matrix, matrix, matrix, matrix),
        out_specs=(both, both, matrix, matrix, matrix, matrix, matrix),
        check_vma=False,
    )
```
